8 devices in a mesh: pp: 2 (over z, y), dp: 4 (over x, core).
Axes of the slice: x: 2, y: 2, z: 1, core: 2. Of those that a mesh axis runs over, the one named last changes fastest.
Arguments:
- act_in: bfloat16 [4, 12, 384, 1536], P(None, 'dp')
- loss_seed: bfloat16 [4, 12, 384, 1536], P(None, 'dp')
- w_qkv: bfloat16 [2, 1536, 48, 96], P('pp', 'dp')
- w_proj: bfloat16 [2, 1536, 1536], P('pp', 'dp')
- w_up: bfloat16 [2, 1536, 6144], P('pp', 'dp')
- w_down: bfloat16 [2, 6144, 1536], P('pp', 'dp')
Outputs:
- output 1: float32 [2, 1536, 48, 96], P('pp', 'dp')
- output 2: float32 [2, 1536, 1536], P('pp', 'dp')
- output 3: float32 [2, 1536, 6144], P('pp', 'dp')
- output 4: float32 [2, 6144, 1536], P('pp', 'dp')
- output 5: bfloat16 [4, 12, 384, 1536], P(None, 'dp', 'pp')
All inputs are finite; a program needn't handle non-finite values.
Results may differ from the reference program's by a relative error of at most 0.0197363.
Values are sent between devices in bfloat16 or wider.
A program may use at most 1 GiB of HBM per device.

```python
import jax
import jax.numpy as jnp
from jax import lax

MICROBATCHES = 4
DP_SIZE = 4
BATCH_DEV = 3
SEQ_LEN = 384
D_MODEL = 1536
NUM_HEADS = 16
TOTAL_LAYERS = 2

HEAD_DIM = D_MODEL // NUM_HEADS
ROWS_ALL = DP_SIZE * BATCH_DEV
NORM_EPS = 1e-6


def setup_inputs(seed: int = 0) -> dict:
    key_list = jax.random.split(jax.random.key(seed), 6)
    act_shape = (MICROBATCHES, ROWS_ALL, SEQ_LEN, D_MODEL)
    seed_scale = (MICROBATCHES * ROWS_ALL * SEQ_LEN) ** -0.5
    act_in = jax.random.normal(key_list[0], act_shape, jnp.float32).astype(jnp.bfloat16)
    loss_seed = (jax.random.normal(key_list[1], act_shape, jnp.float32) * seed_scale).astype(jnp.bfloat16)
    w_qkv = (jax.random.normal(key_list[2], (TOTAL_LAYERS, D_MODEL, 3 * NUM_HEADS, HEAD_DIM), jnp.float32) * D_MODEL ** -0.5).astype(jnp.bfloat16)
    w_proj = (jax.random.normal(key_list[3], (TOTAL_LAYERS, D_MODEL, D_MODEL), jnp.float32) * D_MODEL ** -0.5).astype(jnp.bfloat16)
    w_up = (jax.random.normal(key_list[4], (TOTAL_LAYERS, D_MODEL, 4 * D_MODEL), jnp.float32) * D_MODEL ** -0.5).astype(jnp.bfloat16)
    w_down = (jax.random.normal(key_list[5], (TOTAL_LAYERS, 4 * D_MODEL, D_MODEL), jnp.float32) * (4 * D_MODEL) ** -0.5).astype(jnp.bfloat16)
    return {'act_in': act_in, 'loss_seed': loss_seed, 'w_qkv': w_qkv, 'w_proj': w_proj, 'w_up': w_up, 'w_down': w_down}


def bf16_cast(values):
    return values.astype(jnp.bfloat16).astype(jnp.float32)


def rms_norm(hidden):
    return hidden * lax.rsqrt(jnp.mean(hidden * hidden, axis=-1, keepdims=True) + NORM_EPS)


def layer_apply(hidden, layer_w):
    w_qkv, w_proj, w_up, w_down = layer_w
    hid_f32 = hidden.astype(jnp.float32)
    normed = bf16_cast(rms_norm(hid_f32))
    qkv_act = bf16_cast(jnp.einsum('bsd,dnh->bsnh', normed, w_qkv))
    q_heads = qkv_act[:, :, :NUM_HEADS]
    k_heads = qkv_act[:, :, NUM_HEADS:2 * NUM_HEADS]
    v_heads = qkv_act[:, :, 2 * NUM_HEADS:]
    scores = jnp.einsum('bqnh,bknh->bnqk', q_heads, k_heads) * HEAD_DIM ** -0.5
    causal = jnp.arange(SEQ_LEN)[:, None] >= jnp.arange(SEQ_LEN)[None, :]
    prob_bf = bf16_cast(jax.nn.softmax(jnp.where(causal, scores, -1e30), axis=-1))
    attn_out = bf16_cast(jnp.einsum('bnqk,bknh->bqnh', prob_bf, v_heads))
    attn_flat = attn_out.reshape(hidden.shape)
    mid_f32 = bf16_cast(hid_f32 + jnp.einsum('bse,ed->bsd', attn_flat, w_proj))
    normed2 = bf16_cast(rms_norm(mid_f32))
    up_act = bf16_cast(jnp.einsum('bsd,df->bsf', normed2, w_up))
    gelu_out = bf16_cast(jax.nn.gelu(up_act, approximate=True))
    return (mid_f32 + jnp.einsum('bsf,fd->bsd', gelu_out, w_down)).astype(jnp.bfloat16)


def stack_apply(weight_set, hidden):
    def layer_step(hidden_now, layer_w):
        return layer_apply(hidden_now, layer_w), None
    final_out, _ = lax.scan(jax.checkpoint(layer_step), hidden, weight_set)
    return final_out


def reference(act_in, loss_seed, w_qkv, w_proj, w_up, w_down):
    weights = (w_qkv.astype(jnp.float32), w_proj.astype(jnp.float32), w_up.astype(jnp.float32), w_down.astype(jnp.float32))
    rows_in = act_in.reshape(MICROBATCHES * DP_SIZE, BATCH_DEV, SEQ_LEN, D_MODEL)
    rows_seed = loss_seed.reshape(MICROBATCHES * DP_SIZE, BATCH_DEV, SEQ_LEN, D_MODEL)

    def row_step(grad_sum, row_pair):
        hidden, cotangent = row_pair
        rows_out, pull_back = jax.vjp(lambda weight_set: stack_apply(weight_set, hidden), weights)
        row_grads = pull_back(cotangent)[0]
        return tuple(acc_part + grad_part for acc_part, grad_part in zip(grad_sum, row_grads)), rows_out

    zero_grads = tuple(jnp.zeros_like(w_full) for w_full in weights)
    grad_sum, outs_all = lax.scan(row_step, zero_grads, (rows_in, rows_seed))
    act_out = outs_all.reshape(MICROBATCHES, ROWS_ALL, SEQ_LEN, D_MODEL)
    return grad_sum[0], grad_sum[1], grad_sum[2], grad_sum[3], act_out
```

```python
import functools

import jax
import jax.numpy as jnp
from jax import lax
from jax.experimental import pallas as pl
from jax.experimental.pallas import tpu as pltpu
from jax.sharding import PartitionSpec as P


NORM_EPS = 1e-6
BF16, F32 = jnp.bfloat16, jnp.float32
HEAD = 96
GROUP = 4 * HEAD
LOG2E = 1.4426950408889634
WINDOWS = ((0, 128), (0, 256), (128, 384), (256, 384))


def dot_nn(lhs, rhs):
    return lax.dot_general(lhs, rhs, (((1,), (0,)), ((), ())), preferred_element_type=F32)


def dot_nt(lhs, rhs):
    return lax.dot_general(lhs, rhs, (((1,), (1,)), ((), ())), preferred_element_type=F32)


def dot_tn(lhs, rhs):
    return lax.dot_general(lhs, rhs, (((0,), (0,)), ((), ())), preferred_element_type=F32)


def head_mask(rows, head):
    first, last = WINDOWS[head]
    lane = lax.broadcasted_iota(jnp.int32, (rows, last - first), 1) + first
    return (lane >= head * HEAD) & (lane < (head + 1) * HEAD)


def only(mask, value):
    return jnp.where(mask, value, jnp.zeros_like(value))


def join_windows(parts):
    return jnp.concatenate([
        parts[0] + parts[1][:, :128],
        parts[1][:, 128:] + parts[2][:, :128],
        parts[2][:, 128:] + parts[3],
    ], axis=1)


def attn_fwd_kernel(seq, width, qkv_ref, out_ref):
    scale = HEAD ** -0.5
    block = 128

    def one_group(group, carry):
        first = pl.multiple_of(group * GROUP, 128)
        heads_out = []
        for head in range(4):
            lo, hi = WINDOWS[head]
            q_win = qkv_ref[:, pl.ds(first + lo, hi - lo)]
            mask = head_mask(seq, head)
            k_win = only(mask, qkv_ref[:, pl.ds(width + first + lo, hi - lo)])
            v_win = only(mask, qkv_ref[:, pl.ds(2 * width + first + lo, hi - lo)])
            rows_out = []
            for start in range(0, seq, block):
                keys = start + block
                scores = dot_nt(q_win[start:keys], k_win[:keys])
                row = lax.broadcasted_iota(jnp.int32, (block, keys), 0) + start
                col = lax.broadcasted_iota(jnp.int32, (block, keys), 1)
                scores = jnp.where(row >= col, scores, -1e30)
                top = jnp.max(scores, axis=1, keepdims=True)
                weight = jnp.exp2((scores - top) * (scale * LOG2E))
                prob = weight * (1.0 / jnp.sum(weight, axis=1, keepdims=True))
                rows_out.append(dot_nn(prob.astype(BF16), v_win[:keys]))
            heads_out.append(jnp.concatenate(rows_out, axis=0))
        out_ref[:, pl.ds(first, GROUP)] = join_windows(heads_out).astype(BF16)
        return carry

    lax.fori_loop(0, width // GROUP, one_group, 0)


def attn_bwd_kernel(seq, width, qkv_ref, ct_ref, out_ref):
    scale = HEAD ** -0.5
    blocks = ((0, 256), (256, seq))

    def one_group(group, carry):
        first = pl.multiple_of(group * GROUP, 128)
        ct_q, ct_k, ct_v = [], [], []
        for head in range(4):
            lo, hi = WINDOWS[head]
            mask = head_mask(seq, head)
            q_win = qkv_ref[:, pl.ds(first + lo, hi - lo)]
            ct_win = ct_ref[:, pl.ds(first + lo, hi - lo)]
            q_own, ct_own = only(mask, q_win), only(mask, ct_win)
            k_own = only(mask, qkv_ref[:, pl.ds(width + first + lo, hi - lo)])
            v_own = only(mask, qkv_ref[:, pl.ds(2 * width + first + lo, hi - lo)])
            head_q, head_k, head_v = [], None, None
            for start, stop in blocks:
                keys = stop
                scores = dot_nt(k_own[:keys], q_win[start:stop])
                key = lax.broadcasted_iota(jnp.int32, (keys, stop - start), 0)
                query = lax.broadcasted_iota(jnp.int32, (keys, stop - start), 1) + start
                scores = jnp.where(query >= key, scores, -1e30)
                top = jnp.max(scores, axis=0, keepdims=True)
                weight = jnp.exp2((scores - top) * (scale * LOG2E))
                prob = weight * (1.0 / jnp.sum(weight, axis=0, keepdims=True))
                ct_prob = dot_nt(v_own[:keys], ct_win[start:stop]).astype(BF16).astype(F32)
                inner = prob * ct_prob
                ct_score = ((inner - prob * jnp.sum(inner, axis=0, keepdims=True)) * scale).astype(BF16)
                part_v = dot_nn(prob.astype(BF16), ct_own[start:stop])
                part_k = dot_nn(ct_score, q_own[start:stop])
                head_q.append(dot_tn(ct_score, k_own[:keys]))
                if head_k is None:
                    head_k, head_v = part_k, part_v
                else:
                    old = head_k.shape[0]
                    head_k = jnp.concatenate([head_k + part_k[:old], part_k[old:]], axis=0)
                    head_v = jnp.concatenate([head_v + part_v[:old], part_v[old:]], axis=0)
            ct_q.append(jnp.concatenate(head_q, axis=0))
            ct_k.append(head_k)
            ct_v.append(head_v)
        out_ref[:, pl.ds(first, GROUP)] = join_windows(ct_q).astype(BF16)
        out_ref[:, pl.ds(width + first, GROUP)] = join_windows(ct_k).astype(BF16)
        out_ref[:, pl.ds(2 * width + first, GROUP)] = join_windows(ct_v).astype(BF16)
        return carry

    lax.fori_loop(0, width // GROUP, one_group, 0)


def attention(qkv, seq):
    rows, width = qkv.shape[0], qkv.shape[1] // 3
    flops = 4 * rows * seq * width
    return pl.pallas_call(
        functools.partial(attn_fwd_kernel, seq, width),
        grid=(rows // seq,),
        in_specs=[pl.BlockSpec((seq, 3 * width), lambda i: (i, 0))],
        out_specs=pl.BlockSpec((seq, width), lambda i: (i, 0)),
        out_shape=jax.ShapeDtypeStruct((rows, width), BF16),
        cost_estimate=pl.CostEstimate(flops=flops, bytes_accessed=8 * rows * width, transcendentals=rows * seq * 16),
        compiler_params=pltpu.CompilerParams(vmem_limit_bytes=40 << 20),
        name='attn_fwd',
    )(qkv)


def attention_pull(qkv, ct_heads, seq):
    rows, width = qkv.shape[0], qkv.shape[1] // 3
    flops = 10 * rows * seq * width
    return pl.pallas_call(
        functools.partial(attn_bwd_kernel, seq, width),
        grid=(rows // seq,),
        in_specs=[pl.BlockSpec((seq, 3 * width), lambda i: (i, 0)), pl.BlockSpec((seq, width), lambda i: (i, 0))],
        out_specs=pl.BlockSpec((seq, 3 * width), lambda i: (i, 0)),
        out_shape=jax.ShapeDtypeStruct((rows, 3 * width), BF16),
        cost_estimate=pl.CostEstimate(flops=flops, bytes_accessed=14 * rows * width, transcendentals=rows * seq * 16),
        compiler_params=pltpu.CompilerParams(vmem_limit_bytes=48 << 20),
        name='attn_bwd',
    )(qkv, ct_heads)


def rms_norm(hidden):
    return hidden * lax.rsqrt(jnp.mean(hidden * hidden, axis=-1, keepdims=True) + NORM_EPS)


def rms_pull(hidden, ct_normed):
    return jax.vjp(rms_norm, hidden.astype(F32))[1](ct_normed.astype(F32))[0]


def gelu_tanh(pre_act):
    return jax.nn.gelu(pre_act, approximate=True)


def block_forward(hidden, weights, seq):
    w_qkv, w_proj, w_up, _ = weights
    hid_f32 = hidden.astype(F32)
    normed = rms_norm(hid_f32).astype(BF16)
    qkv = dot_nn(normed, w_qkv).astype(BF16)
    heads = attention(qkv, seq)
    mid = (hid_f32 + dot_nn(heads, w_proj)).astype(BF16)
    normed2 = rms_norm(mid.astype(F32)).astype(BF16)
    up_act = dot_nn(normed2, w_up).astype(BF16)
    gelu_out = gelu_tanh(up_act.astype(F32)).astype(BF16)
    return hidden, normed, qkv, heads, mid, normed2, up_act, gelu_out


def block_output(saved, w_down):
    return (saved[4].astype(F32) + dot_nn(saved[7], w_down)).astype(BF16)


def block_backward(saved, ct_out, weights, seq, tag):
    w_qkv, w_proj, w_up, w_down = weights
    hidden, normed, qkv, heads, mid, normed2, up_act, gelu_out = saved
    g_down, ct_out = lax.optimization_barrier((dot_tn(gelu_out, ct_out), ct_out))
    ct_gelu = dot_nt(ct_out, w_down).astype(BF16)
    ct_up = jax.vjp(gelu_tanh, up_act.astype(F32))[1](ct_gelu.astype(F32))[0].astype(BF16)
    g_up, ct_up = lax.optimization_barrier((dot_tn(normed2, ct_up), ct_up))
    ct_norm2 = dot_nt(ct_up, w_up).astype(BF16)
    ct_mid = (ct_out.astype(F32) + rms_pull(mid, ct_norm2)).astype(BF16)
    g_proj, ct_mid = lax.optimization_barrier((dot_tn(heads, ct_mid), ct_mid))
    ct_heads = dot_nt(ct_mid, w_proj).astype(BF16)
    ct_qkv = attention_pull(qkv, ct_heads, seq)
    g_qkv, ct_qkv = lax.optimization_barrier((dot_tn(normed, ct_qkv), ct_qkv))
    ct_hidden = None
    if tag:
        ct_norm = dot_nt(ct_qkv, w_qkv).astype(BF16)
        ct_hidden = (ct_mid.astype(F32) + rms_pull(hidden, ct_norm)).astype(BF16)
    return ct_hidden, (g_qkv, g_proj, g_up, g_down)


def solution(mesh):
    swap = [(0, 1), (1, 0)]
    both = ('dp', 'pp')

    def whole_step(act_in, loss_seed, w_qkv, w_proj, w_up, w_down):
        row = lax.axis_index('pp')
        num_micro, batch, seq, width = act_in.shape
        half_micro = num_micro // 2

        def mine(array):
            return lax.dynamic_slice_in_dim(array, row * half_micro, half_micro, 0).reshape(-1, width)

        def halves(shard):
            half = shard.shape[0] // 2
            kept = lax.dynamic_slice_in_dim(shard, row * half, half, 0)
            sent = lax.dynamic_slice_in_dim(shard, (1 - row) * half, half, 0)
            got = lax.ppermute(sent, 'pp', swap)
            return jnp.where(row == 0, kept, got), jnp.where(row == 0, got, kept)

        def gather(part):
            return lax.all_gather(part, both, axis=0, tiled=True)

        shard_qkv = w_qkv[0].reshape(w_qkv.shape[1], -1)
        qkv_both = lax.all_gather(shard_qkv, ('pp', 'dp'), axis=0, tiled=True)
        parts = [halves(shard[0]) for shard in (w_proj, w_up, w_down)]
        weights = []
        for idx in range(2):
            weights.append((qkv_both[idx * width:(idx + 1) * width],) + tuple(gather(part[idx]) for part in parts))

        hidden, seed = mine(act_in), mine(loss_seed)
        saved0 = block_forward(hidden, weights[0], seq)
        hidden1 = block_output(saved0, weights[0][3])
        saved1 = block_forward(hidden1, weights[1], seq)
        ct_mid, grads1 = block_backward(saved1, seed, weights[1], seq, 1)
        _, grads0 = block_backward(saved0, ct_mid, weights[0], seq, 0)
        out = block_output(saved1, weights[1][3]).reshape(half_micro, batch, seq, width)

        def reduce(grad):
            return lax.psum_scatter(grad, both, scatter_dimension=0, tiled=True)

        sums1 = [reduce(grads1[i]) for i in (3, 2, 1, 0)]
        sums0 = [reduce(grads0[i]) for i in (3, 2, 1, 0)]

        def settle(sum0, sum1):
            kept = jnp.where(row == 0, sum0, sum1)
            got = lax.ppermute(jnp.where(row == 0, sum1, sum0), 'pp', swap)
            return lax.dynamic_update_slice_in_dim(jnp.concatenate([kept, kept]), got, (1 - row) * got.shape[0], 0)

        g_down, g_up, g_proj, g_qkv = [settle(sum0, sum1)[None] for sum0, sum1 in zip(sums0, sums1)]

        half = seq // 2
        kept = lax.dynamic_slice_in_dim(out, row * half, half, 2)
        got = lax.ppermute(lax.dynamic_slice_in_dim(out, (1 - row) * half, half, 2), 'pp', swap)
        act_out = lax.dynamic_update_slice_in_dim(jnp.concatenate([kept, kept]), got, (1 - row) * half_micro, 0)
        return g_qkv.reshape(w_qkv.shape), g_proj, g_up, g_down, act_out

    weight_spec = P('pp', 'dp')
    act_spec = P(None, 'dp')
    return jax.shard_map(whole_step, mesh=mesh, in_specs=(act_spec, act_spec, weight_spec, weight_spec, weight_spec, weight_spec), out_specs=(weight_spec, weight_spec, weight_spec, weight_spec, P(None, 'dp', 'pp')), check_vma=False)
```
